32 devices in a mesh: lat: 8 (over z, y), lon: 4 (over x, core).
Axes of the slice: x: 2, y: 2, z: 4, core: 2. Of those that a mesh axis runs over, the one named last changes fastest.
Arguments:
- raw_fields: bfloat16 [32, 160, 1440], P(('lat', 'lon')), may hold values from -6 to 6
- embed_weight: bfloat16 [32, 4, 4, 1024], replicated, may hold values from -0.25 to 0.25
- embed_bias: float32 [1024], replicated, may hold values from -3 to 3
- conv_weight: bfloat16 [3, 3, 1024, 1024], replicated, may hold values from -0.0625 to 0.0625
- conv_bias: float32 [1024], replicated, may hold values from -3 to 3
Outputs:
- features: bfloat16 [40, 360, 1024], P('lat', 'lon')
The draws below stay inside these ranges and needn't reach their ends.
All inputs are finite; a program needn't handle non-finite values.
Results may differ from the reference program's by a relative error of at most 0.0049.
Values may be sent and summed in bfloat16 or wider, within the bound.
No kernel may reach another device: no remote copies, remote signals or barrier semaphores. Data moves between devices by JAX's collectives and lax.ppermute only.
A program may use at most 192 MiB of HBM per device.

```python
import jax
import jax.numpy as jnp

PATCH = 4
WIDTH = 1024
VARS = 32
HEIGHT = 160
BREADTH = 1440


def shard_levels(key, extent, split, least, top_value):
    level = 1.0
    for dim, shards_of in split:
        heights = jax.random.uniform(jax.random.fold_in(jax.random.fold_in(key, 6), dim), (shards_of,), jnp.float32, least / len(split), top_value / len(split))
        level = level * jnp.repeat(jnp.exp(heights), extent[dim] // shards_of).reshape((-1,) + (1,) * (len(extent) - 1 - dim))
    return level


def gaussian(own_key, dims, scale, most, pieces=(), kind=jnp.bfloat16):
    gain = shard_levels(own_key, dims, pieces, -0.22, 0.18) if pieces else 1.0
    values = jax.random.normal(own_key, dims, jnp.float32) * scale * gain
    return jnp.minimum(jnp.maximum(values, -most), most).astype(kind)


def setup_inputs(seed: int = 0) -> dict:
    arg_keys = jax.random.split(jax.random.key(seed), 6)
    return {
        "raw_fields": gaussian(arg_keys[0], (VARS, HEIGHT, BREADTH), 1.0, 6.0, ((0, 32),)),
        "embed_weight": gaussian(arg_keys[1], (VARS, PATCH, PATCH, WIDTH), (VARS * PATCH * PATCH) ** -0.5, 0.25),
        "embed_bias": gaussian(arg_keys[2], (WIDTH,), 0.5, 3.0, (), jnp.float32),
        "conv_weight": gaussian(arg_keys[3], (3, 3, WIDTH, WIDTH), (9 * WIDTH) ** -0.5, 0.0625),
        "conv_bias": gaussian(arg_keys[4], (WIDTH,), 0.5, 3.0, (), jnp.float32),
    }


def reference(raw_fields, embed_weight, embed_bias, conv_weight, conv_bias):
    count, height, breadth = raw_fields.shape
    patch_rows = height // PATCH
    patch_cols = breadth // PATCH
    grid_blocks = raw_fields.astype(jnp.float32).reshape(count, patch_rows, PATCH, patch_cols, PATCH)
    embedded = jnp.einsum("vaibj,vijd->abd", grid_blocks, embed_weight.astype(jnp.float32))
    embedded = (embedded + embed_bias).astype(jnp.bfloat16)
    channels = embedded.shape[2]
    padded = jnp.pad(embedded, ((0, 0), (1, 1), (0, 0)), mode="wrap")
    padded = jnp.pad(padded, ((1, 1), (0, 0), (0, 0)))
    summed = jnp.zeros((patch_rows * patch_cols, channels), jnp.float32)
    for step_row in range(3):
        for step_col in range(3):
            window = padded[step_row:step_row + patch_rows, step_col:step_col + patch_cols].reshape(-1, channels)
            summed = summed + jnp.dot(window, conv_weight[step_row, step_col], preferred_element_type=jnp.float32)
    summed = summed + conv_bias
    result = jax.nn.gelu(summed, approximate=False).astype(jnp.bfloat16)
    return result.reshape(patch_rows, patch_cols, channels)
```

```python
import functools

import jax
import jax.numpy as jnp
from jax import lax
from jax.experimental import pallas as pl
from jax.experimental.pallas import tpu as pltpu
from jax.sharding import PartitionSpec as P

PATCH = 4
LANES = 128


def with_halo(value, sides, width, wrap):
    for axis, dim in sides:
        count, length = (lax.axis_size(axis), value.shape[dim])
        up = [(i, (i + 1) % count) for i in range(count if wrap else count - 1)]
        down = [(j, i) for i, j in up]
        last = lax.slice_in_dim(value, length - width, length, axis=dim)
        leading = lax.slice_in_dim(value, 0, width, axis=dim)
        before = lax.ppermute(last, axis, up)
        after = lax.ppermute(leading, axis, down)
        value = jnp.concatenate([before, value, after], axis=dim)
    return value


def two_stages(raw_fields, embed_weight, embed_bias, conv_weight, conv_bias):
    lat_count = lax.axis_size("lat")
    lon_count = lax.axis_size("lon")
    var_dev, height, breadth = raw_fields.shape
    tile_height = height // lat_count
    tile_breadth = breadth // lon_count
    pieces = raw_fields.reshape(var_dev, lat_count, tile_height, lon_count, tile_breadth)
    pieces = pieces.transpose(1, 3, 0, 2, 4).reshape(
        lat_count * lon_count * var_dev, tile_height, tile_breadth
    )
    tile_block = lax.all_to_all(pieces, ("lat", "lon"), split_axis=0, concat_axis=0, tiled=True)
    patch_rows = tile_height // PATCH
    patch_cols = tile_breadth // PATCH
    grid_blocks = tile_block.reshape(-1, patch_rows, PATCH, patch_cols, PATCH)
    embedded = jnp.einsum(
        "vaibj,vijd->abd", grid_blocks, embed_weight, preferred_element_type=jnp.float32
    )
    embedded = (embedded + embed_bias).astype(jnp.bfloat16)
    channels = embedded.shape[2]
    lon_padded = with_halo(embedded, (("lon", 1),), 1, True)
    padded = with_halo(lon_padded, (("lat", 0),), 1, False)
    summed = jnp.zeros((patch_rows * patch_cols, channels), jnp.float32)
    for step_row in range(3):
        for step_col in range(3):
            window = padded[
                step_row : step_row + patch_rows, step_col : step_col + patch_cols
            ].reshape(-1, channels)
            summed = summed + jnp.dot(
                window, conv_weight[step_row, step_col], preferred_element_type=jnp.float32
            )
    summed = summed + conv_bias
    result = jax.nn.gelu(summed, approximate=False).astype(jnp.bfloat16)
    return result.reshape(patch_rows, patch_cols, channels)


def windows_kernel(raw_ref, out_ref, *, lat_count, lon_count, tile_rows, tile_breadth):
    height, breadth = raw_ref.shape[1:]
    span = tile_breadth + 2 * PATCH
    patches_high = height // PATCH
    rows = tile_rows + 2
    raw = raw_ref[0]
    for lon in range(lon_count):
        first = lon * tile_breadth - PATCH
        last = first + span
        if first < 0:
            window = jnp.concatenate([raw[:, first:], raw[:, :last]], axis=1)
        elif last > breadth:
            window = jnp.concatenate([raw[:, first:], raw[:, : last - breadth]], axis=1)
        else:
            window = raw[:, first:last]
        for patch_row in range(patches_high):
            piece = window[PATCH * patch_row : PATCH * (patch_row + 1)]
            for lat in range(lat_count):
                for step in range(rows):
                    wanted = lat * tile_rows - 1 + step
                    if min(max(wanted, 0), patches_high - 1) == patch_row:
                        out_ref[lat * lon_count + lon, step] = piece


def compose_kernel(embed_ref, bias_ref, conv_ref, weight_ref, shift_ref):
    weight_ref[0] = jnp.dot(
        embed_ref[...], conv_ref[0], preferred_element_type=jnp.float32
    ).astype(weight_ref.dtype)
    rest = bias_ref[...]
    shift = None
    for _ in range(3):
        part = rest.astype(conv_ref.dtype)
        rest = rest - part.astype(jnp.float32)
        term = jnp.dot(part, conv_ref[0], preferred_element_type=jnp.float32)
        shift = term if shift is None else shift + term
    shift_ref[0] = shift


def tokens_kernel(
    edge_ref, tile_ref, weight_ref, bias_ref, out_ref, turned_ref, cells_ref, *, pitch, block
):
    variables, rows, _, span = tile_ref.shape
    tile_rows, tile_cols, channels = out_ref.shape
    depth = variables * PATCH
    steps = 3 * PATCH
    for row in range(rows):
        cells = tile_ref[:, row].astype(jnp.float32).reshape(depth, span)
        if row == 0:
            cells = cells * edge_ref[0]
        if row == rows - 1:
            cells = cells * edge_ref[1]
        turned_ref[row, :span] = cells.T
        for step in range(steps):
            picked = turned_ref[row, pl.ds(step, pitch, stride=PATCH), :]
            cells_ref[row * pitch : (row + 1) * pitch, step * depth : (step + 1) * depth] = (
                picked.astype(cells_ref.dtype)
            )
    many = tile_rows * pitch
    for first in range(0, channels, block):
        total = None
        for tap_row in range(3):
            part = jnp.dot(
                cells_ref[tap_row * pitch : tap_row * pitch + many],
                weight_ref[
                    tap_row * steps * depth : (tap_row + 1) * steps * depth, first : first + block
                ],
                preferred_element_type=jnp.float32,
            )
            total = part if total is None else total + part
        for row in range(tile_rows):
            kind = 0 if row == 0 else 2 if row == tile_rows - 1 else 1
            value = total[row * pitch : row * pitch + tile_cols]
            value = value + bias_ref[kind : kind + 1, first : first + block]
            value = 0.5 * value * (1.0 + lax.erf(value * (0.5**0.5)))
            out_ref[row, :, first : first + block] = value.astype(out_ref.dtype)


def one_stage(raw_fields, embed_weight, embed_bias, conv_weight, conv_bias):
    lat_count = lax.axis_size("lat")
    lon_count = lax.axis_size("lon")
    devices = lat_count * lon_count
    _, height, breadth = raw_fields.shape
    variables, _, _, channels = embed_weight.shape
    tile_rows = height // lat_count // PATCH
    tile_breadth = breadth // lon_count
    tile_cols = tile_breadth // PATCH
    rows = tile_rows + 2
    span = tile_breadth + 2 * PATCH
    depth = variables * PATCH
    cells = depth * PATCH
    pitch = -(-(tile_cols + 2) // 16) * 16
    lowest = jnp.bfloat16

    pieces = pl.pallas_call(
        functools.partial(
            windows_kernel,
            lat_count=lat_count,
            lon_count=lon_count,
            tile_rows=tile_rows,
            tile_breadth=tile_breadth,
        ),
        out_shape=jax.ShapeDtypeStruct((devices, rows, PATCH, span), lowest),
        name="windows",
    )(raw_fields)
    tile = lax.all_to_all(pieces, ("lat", "lon"), split_axis=0, concat_axis=0, tiled=True)

    turned = embed_weight.transpose(2, 0, 1, 3).reshape(cells, channels)
    bias_rows = jnp.broadcast_to(embed_bias, (8, channels))
    taps = conv_weight.reshape(9, channels, channels)
    weight, shift = pl.pallas_call(
        compose_kernel,
        grid=(9,),
        in_specs=[
            pl.BlockSpec((cells, channels), lambda t: (0, 0)),
            pl.BlockSpec((8, channels), lambda t: (0, 0)),
            pl.BlockSpec((1, channels, channels), lambda t: (t, 0, 0)),
        ],
        out_specs=[
            pl.BlockSpec((1, cells, channels), lambda t: (t, 0, 0)),
            pl.BlockSpec((1, 8, channels), lambda t: (t, 0, 0)),
        ],
        out_shape=[
            jax.ShapeDtypeStruct((9, cells, channels), lowest),
            jax.ShapeDtypeStruct((9, 8, channels), jnp.float32),
        ],
        name="compose",
    )(turned, bias_rows, taps)
    row_shift = shift[:, 0].reshape(3, 3, channels).sum(axis=1)
    lat = lax.axis_index("lat")
    above = jnp.where(lat > 0, 1.0, 0.0).astype(jnp.float32)
    below = jnp.where(lat < lat_count - 1, 1.0, 0.0).astype(jnp.float32)
    middle = conv_bias + row_shift[1]
    both = middle + row_shift[0] + row_shift[2]
    top = middle + above * row_shift[0] + row_shift[2]
    bottom = middle + row_shift[0] + below * row_shift[2]
    biases = jnp.stack([top, both, bottom])
    edges = jnp.stack([above, below])

    return pl.pallas_call(
        functools.partial(tokens_kernel, pitch=pitch, block=2 * LANES),
        in_specs=[
            pl.BlockSpec(memory_space=pltpu.SMEM),
            pl.BlockSpec(memory_space=pltpu.VMEM),
            pl.BlockSpec(memory_space=pltpu.VMEM),
            pl.BlockSpec(memory_space=pltpu.VMEM),
        ],
        out_specs=pl.BlockSpec(memory_space=pltpu.VMEM),
        out_shape=jax.ShapeDtypeStruct((tile_rows, tile_cols, channels), lowest),
        scratch_shapes=[
            pltpu.VMEM((rows, PATCH * pitch + 3 * PATCH, depth), jnp.float32),
            pltpu.VMEM((rows * pitch, 3 * cells), lowest),
        ],
        name="tokens",
    )(edges, tile, weight.reshape(9 * cells, channels), biases)


def per_device(raw_fields, embed_weight, embed_bias, conv_weight, conv_bias):
    variables, _, _, channels = embed_weight.shape
    if raw_fields.shape[0] == 1 and variables * PATCH * PATCH <= channels:
        return one_stage(raw_fields, embed_weight, embed_bias, conv_weight, conv_bias)
    return two_stages(raw_fields, embed_weight, embed_bias, conv_weight, conv_bias)


def solution(mesh):
    return jax.shard_map(
        per_device,
        mesh=mesh,
        in_specs=(P(("lat", "lon"), None, None), P(), P(), P(), P()),
        out_specs=P("lat", "lon", None),
        check_vma=False,
    )
```

```python
import functools

import jax
import jax.numpy as jnp
from jax import lax
from jax.experimental import pallas as pl
from jax.experimental.pallas import tpu as pltpu
from jax.sharding import PartitionSpec as P

PATCH = 4
LANES = 128


def with_halo(value, sides, width, wrap):
    for axis, dim in sides:
        count, length = (lax.axis_size(axis), value.shape[dim])
        up = [(i, (i + 1) % count) for i in range(count if wrap else count - 1)]
        down = [(j, i) for i, j in up]
        last = lax.slice_in_dim(value, length - width, length, axis=dim)
        leading = lax.slice_in_dim(value, 0, width, axis=dim)
        before = lax.ppermute(last, axis, up)
        after = lax.ppermute(leading, axis, down)
        value = jnp.concatenate([before, value, after], axis=dim)
    return value


def two_stages(raw_fields, embed_weight, embed_bias, conv_weight, conv_bias):
    lat_count = lax.axis_size("lat")
    lon_count = lax.axis_size("lon")
    var_dev, height, breadth = raw_fields.shape
    tile_height = height // lat_count
    tile_breadth = breadth // lon_count
    pieces = raw_fields.reshape(var_dev, lat_count, tile_height, lon_count, tile_breadth)
    pieces = pieces.transpose(1, 3, 0, 2, 4).reshape(
        lat_count * lon_count * var_dev, tile_height, tile_breadth
    )
    tile_block = lax.all_to_all(pieces, ("lat", "lon"), split_axis=0, concat_axis=0, tiled=True)
    patch_rows = tile_height // PATCH
    patch_cols = tile_breadth // PATCH
    grid_blocks = tile_block.reshape(-1, patch_rows, PATCH, patch_cols, PATCH)
    embedded = jnp.einsum(
        "vaibj,vijd->abd", grid_blocks, embed_weight, preferred_element_type=jnp.float32
    )
    embedded = (embedded + embed_bias).astype(jnp.bfloat16)
    channels = embedded.shape[2]
    lon_padded = with_halo(embedded, (("lon", 1),), 1, True)
    padded = with_halo(lon_padded, (("lat", 0),), 1, False)
    summed = jnp.zeros((patch_rows * patch_cols, channels), jnp.float32)
    for step_row in range(3):
        for step_col in range(3):
            window = padded[
                step_row : step_row + patch_rows, step_col : step_col + patch_cols
            ].reshape(-1, channels)
            summed = summed + jnp.dot(
                window, conv_weight[step_row, step_col], preferred_element_type=jnp.float32
            )
    summed = summed + conv_bias
    result = jax.nn.gelu(summed, approximate=False).astype(jnp.bfloat16)
    return result.reshape(patch_rows, patch_cols, channels)


def windows_kernel(raw_ref, out_ref, *, lat_count, lon_count, tile_rows, tile_breadth):
    height, breadth = raw_ref.shape[1:]
    span = tile_breadth + 2 * PATCH
    patches_high = height // PATCH
    rows = tile_rows + 2
    raw = raw_ref[0]
    for lon in range(lon_count):
        first = lon * tile_breadth - PATCH
        last = first + span
        if first < 0:
            window = jnp.concatenate([raw[:, first:], raw[:, :last]], axis=1)
        elif last > breadth:
            window = jnp.concatenate([raw[:, first:], raw[:, : last - breadth]], axis=1)
        else:
            window = raw[:, first:last]
        for patch_row in range(patches_high):
            piece = window[PATCH * patch_row : PATCH * (patch_row + 1)]
            for lat in range(lat_count):
                for step in range(rows):
                    wanted = lat * tile_rows - 1 + step
                    if min(max(wanted, 0), patches_high - 1) == patch_row:
                        out_ref[lat * lon_count + lon, step] = piece


def compose_kernel(
    embed_ref,
    bias_ref,
    conv_hbm,
    near_ref,
    far_hbm,
    shift_ref,
    plain_ref,
    left_ref,
    taps_ref,
    made_ref,
    arrived,
    left,
):
    taps = conv_hbm.shape[0]
    near = near_ref.shape[0]
    parts, cells, _ = plain_ref.shape
    depth = cells // PATCH
    rim = left_ref.shape[0] - cells

    def fetch(tap):
        return pltpu.make_async_copy(conv_hbm.at[tap], taps_ref.at[tap], arrived.at[tap])

    def send(tap):
        return pltpu.make_async_copy(made_ref.at[tap], far_hbm.at[tap], left.at[tap])

    for tap in range(taps):
        fetch(tap).start()
    rest = bias_ref[...]
    lines = lax.broadcasted_iota(jnp.int32, (rim, rest.shape[1]), 0)
    below = jnp.zeros(lines.shape, jnp.float32)
    for line in range(3):
        part = rest.astype(left_ref.dtype).astype(jnp.float32)
        below = jnp.where(lines == line, part, below)
        rest = rest - part
    left_ref[cells:] = below.astype(left_ref.dtype)
    for part in range(parts):
        lanes = slice(part * LANES, (part + 1) * LANES)
        plain_ref[part] = embed_ref[..., lanes].astype(jnp.float32).reshape(cells, LANES)
        for step in range(PATCH):
            left_ref[step * depth : (step + 1) * depth, lanes] = plain_ref[
                part, pl.ds(step, depth, stride=PATCH), :
            ].astype(left_ref.dtype)
    shift_ref[...] = jnp.zeros_like(shift_ref)

    def compose(tap, keep):
        fetch(tap).wait()
        both = jnp.dot(left_ref[...], taps_ref[tap], preferred_element_type=jnp.float32)
        shift_ref[tap // 3] += jnp.broadcast_to(
            both[cells:].sum(axis=0, keepdims=True), shift_ref.shape[1:]
        )
        keep(both[:cells].astype(far_hbm.dtype))

    def compose_near(tap, carry):
        def keep(value):
            near_ref[tap] = value

        compose(tap, keep)
        return carry

    def compose_far(tap, carry):
        def keep(value):
            made_ref[tap] = value
            send(tap).start()

        compose(tap + near, keep)
        return carry

    lax.fori_loop(0, near, compose_near, None)
    lax.fori_loop(0, taps - near, compose_far, None)
    for tap in range(taps - near):
        send(tap).wait()


def tokens_kernel(
    tile_ref,
    near_ref,
    far_hbm,
    shift_ref,
    bias_ref,
    out_ref,
    far_ref,
    turned_ref,
    cells_ref,
    total_ref,
    arrived,
    *,
    pitch,
    block,
):
    variables, rows, _, span = tile_ref.shape
    tile_rows, tile_cols, channels = out_ref.shape
    depth = variables * PATCH
    cells = depth * PATCH
    steps = 3 * PATCH
    near = near_ref.shape[0]
    bounds = (0, 3 - near, 6 - near, 9 - near)

    def fetch(tap_row):
        taps = pl.ds(bounds[tap_row], bounds[tap_row + 1] - bounds[tap_row])
        return pltpu.make_async_copy(far_hbm.at[taps], far_ref.at[taps], arrived.at[tap_row])

    for tap_row in range(3):
        fetch(tap_row).start()
    lat = lax.axis_index("lat")
    above = jnp.where(lat > 0, 1.0, 0.0).astype(jnp.float32)
    below = jnp.where(lat < lax.axis_size("lat") - 1, 1.0, 0.0).astype(jnp.float32)
    for row in range(rows):
        tile = tile_ref[:, row].astype(jnp.float32).reshape(depth, span)
        if row == 0:
            tile = tile * above
        if row == rows - 1:
            tile = tile * below
        turned_ref[row, :span] = tile.T
        for step in range(steps):
            picked = turned_ref[row, pl.ds(step, pitch, stride=PATCH), :]
            cells_ref[row * pitch : (row + 1) * pitch, step * depth : (step + 1) * depth] = (
                picked.astype(cells_ref.dtype)
            )

    def product(tap_row, first, weight):
        count = weight.shape[0]
        left = cells_ref[
            tap_row * pitch : (tap_row + tile_rows) * pitch, first * cells : (first + count) * cells
        ]
        right = weight.reshape(count * cells, weight.shape[2])
        return jnp.dot(left, right, preferred_element_type=jnp.float32)

    total_ref[...] = product(0, 0, near_ref[...])
    fetch(0).wait()
    total_ref[...] += product(0, near, far_ref[bounds[0] : bounds[1]])
    fetch(1).wait()
    total_ref[...] += product(1, 0, far_ref[bounds[1] : bounds[2]])
    fetch(2).wait()
    for first in range(0, channels, block):
        lanes = slice(first, first + block)
        total = total_ref[:, lanes] + product(2, 0, far_ref[bounds[2] : bounds[3], :, lanes])
        for row in range(tile_rows):
            bias = bias_ref[:, lanes] + shift_ref[1, :1, lanes]
            over = shift_ref[0, :1, lanes]
            under = shift_ref[2, :1, lanes]
            bias = bias + (over * above if row == 0 else over)
            bias = bias + (under * below if row == tile_rows - 1 else under)
            value = total[row * pitch : row * pitch + tile_cols] + bias
            value = 0.5 * value * (1.0 + lax.erf(value * (0.5**0.5)))
            out_ref[row, :, lanes] = value.astype(out_ref.dtype)


def one_stage(raw_fields, embed_weight, embed_bias, conv_weight, conv_bias):
    lat_count = lax.axis_size("lat")
    lon_count = lax.axis_size("lon")
    devices = lat_count * lon_count
    _, height, breadth = raw_fields.shape
    variables, _, _, channels = embed_weight.shape
    tile_rows = height // lat_count // PATCH
    tile_breadth = breadth // lon_count
    tile_cols = tile_breadth // PATCH
    rows = tile_rows + 2
    span = tile_breadth + 2 * PATCH
    depth = variables * PATCH
    cells = depth * PATCH
    pitch = -(-(tile_cols + 2) // 16) * 16
    lowest = jnp.bfloat16

    pieces = pl.pallas_call(
        functools.partial(
            windows_kernel,
            lat_count=lat_count,
            lon_count=lon_count,
            tile_rows=tile_rows,
            tile_breadth=tile_breadth,
        ),
        out_shape=pltpu.VMEM((devices, rows, PATCH, span), lowest),
        name="windows",
    )(raw_fields)
    tile = lax.all_to_all(pieces, ("lat", "lon"), split_axis=0, concat_axis=0, tiled=True)

    whole = pl.BlockSpec(memory_space=pltpu.VMEM)
    afar = pl.BlockSpec(memory_space=pl.ANY)
    taps, near = 9, 2
    close, far, shift = pl.pallas_call(
        compose_kernel,
        in_specs=[whole, whole, afar],
        out_specs=[whole, afar, whole],
        out_shape=[
            pltpu.VMEM((near, cells, channels), lowest),
            jax.ShapeDtypeStruct((taps - near, cells, channels), lowest),
            pltpu.VMEM((3, 8, channels), jnp.float32),
        ],
        scratch_shapes=[
            pltpu.VMEM((channels // LANES, cells, LANES), jnp.float32),
            pltpu.VMEM((cells + 16, channels), lowest),
            pltpu.VMEM((taps, channels, channels), lowest),
            pltpu.VMEM((taps - near, cells, channels), lowest),
            pltpu.SemaphoreType.DMA((taps,)),
            pltpu.SemaphoreType.DMA((taps - near,)),
        ],
        compiler_params=pltpu.CompilerParams(vmem_limit_bytes=48 << 20),
        name="compose",
    )(
        pltpu.with_memory_space_constraint(embed_weight, pltpu.VMEM),
        embed_bias.reshape(1, channels),
        conv_weight.reshape(taps, channels, channels),
    )

    return pl.pallas_call(
        functools.partial(tokens_kernel, pitch=pitch, block=4 * LANES),
        in_specs=[whole, whole, afar, whole, whole],
        out_specs=whole,
        out_shape=jax.ShapeDtypeStruct((tile_rows, tile_cols, channels), lowest),
        scratch_shapes=[
            pltpu.VMEM((taps - near, cells, channels), lowest),
            pltpu.VMEM((rows, PATCH * pitch + 3 * PATCH, depth), jnp.float32),
            pltpu.VMEM((rows * pitch, 3 * cells), lowest),
            pltpu.VMEM((tile_rows * pitch, channels), jnp.float32),
            pltpu.SemaphoreType.DMA((3,)),
        ],
        compiler_params=pltpu.CompilerParams(vmem_limit_bytes=32 << 20),
        name="tokens",
    )(
        pltpu.with_memory_space_constraint(tile, pltpu.VMEM),
        pltpu.with_memory_space_constraint(close, pltpu.VMEM),
        pltpu.with_memory_space_constraint(far, pltpu.HBM),
        pltpu.with_memory_space_constraint(shift, pltpu.VMEM),
        conv_bias.reshape(1, channels),
    )


def per_device(raw_fields, embed_weight, embed_bias, conv_weight, conv_bias):
    variables, _, _, channels = embed_weight.shape
    if raw_fields.shape[0] == 1 and variables * PATCH * PATCH <= channels:
        return one_stage(raw_fields, embed_weight, embed_bias, conv_weight, conv_bias)
    return two_stages(raw_fields, embed_weight, embed_bias, conv_weight, conv_bias)


def solution(mesh):
    return jax.shard_map(
        per_device,
        mesh=mesh,
        in_specs=(P(("lat", "lon"), None, None), P(), P(), P(), P()),
        out_specs=P("lat", "lon", None),
        check_vma=False,
    )
```

```python
import functools

import jax
import jax.numpy as jnp
from jax import lax
from jax.experimental import pallas as pl
from jax.experimental.pallas import tpu as pltpu
from jax.sharding import PartitionSpec as P

PATCH = 4
LANES = 128


def with_halo(value, sides, width, wrap):
    for axis, dim in sides:
        count, length = (lax.axis_size(axis), value.shape[dim])
        up = [(i, (i + 1) % count) for i in range(count if wrap else count - 1)]
        down = [(j, i) for i, j in up]
        last = lax.slice_in_dim(value, length - width, length, axis=dim)
        leading = lax.slice_in_dim(value, 0, width, axis=dim)
        before = lax.ppermute(last, axis, up)
        after = lax.ppermute(leading, axis, down)
        value = jnp.concatenate([before, value, after], axis=dim)
    return value


def two_stages(raw_fields, embed_weight, embed_bias, conv_weight, conv_bias):
    lat_count = lax.axis_size("lat")
    lon_count = lax.axis_size("lon")
    var_dev, height, breadth = raw_fields.shape
    tile_height = height // lat_count
    tile_breadth = breadth // lon_count
    pieces = raw_fields.reshape(var_dev, lat_count, tile_height, lon_count, tile_breadth)
    pieces = pieces.transpose(1, 3, 0, 2, 4).reshape(
        lat_count * lon_count * var_dev, tile_height, tile_breadth
    )
    tile_block = lax.all_to_all(pieces, ("lat", "lon"), split_axis=0, concat_axis=0, tiled=True)
    patch_rows = tile_height // PATCH
    patch_cols = tile_breadth // PATCH
    grid_blocks = tile_block.reshape(-1, patch_rows, PATCH, patch_cols, PATCH)
    embedded = jnp.einsum(
        "vaibj,vijd->abd", grid_blocks, embed_weight, preferred_element_type=jnp.float32
    )
    embedded = (embedded + embed_bias).astype(jnp.bfloat16)
    channels = embedded.shape[2]
    lon_padded = with_halo(embedded, (("lon", 1),), 1, True)
    padded = with_halo(lon_padded, (("lat", 0),), 1, False)
    summed = jnp.zeros((patch_rows * patch_cols, channels), jnp.float32)
    for step_row in range(3):
        for step_col in range(3):
            window = padded[
                step_row : step_row + patch_rows, step_col : step_col + patch_cols
            ].reshape(-1, channels)
            summed = summed + jnp.dot(
                window, conv_weight[step_row, step_col], preferred_element_type=jnp.float32
            )
    summed = summed + conv_bias
    result = jax.nn.gelu(summed, approximate=False).astype(jnp.bfloat16)
    return result.reshape(patch_rows, patch_cols, channels)


def windows_kernel(raw_ref, out_ref, *, lat_count, lon_count, tile_rows, tile_breadth):
    height, breadth = raw_ref.shape[1:]
    span = tile_breadth + 2 * PATCH
    patches_high = height // PATCH
    rows = tile_rows + 2
    raw = raw_ref[0]
    for lon in range(lon_count):
        first = lon * tile_breadth - PATCH
        last = first + span
        if first < 0:
            window = jnp.concatenate([raw[:, first:], raw[:, :last]], axis=1)
        elif last > breadth:
            window = jnp.concatenate([raw[:, first:], raw[:, : last - breadth]], axis=1)
        else:
            window = raw[:, first:last]
        for patch_row in range(patches_high):
            piece = window[PATCH * patch_row : PATCH * (patch_row + 1)]
            for lat in range(lat_count):
                for step in range(rows):
                    wanted = lat * tile_rows - 1 + step
                    if min(max(wanted, 0), patches_high - 1) == patch_row:
                        out_ref[lat * lon_count + lon, step] = piece


def compose_kernel(
    embed_ref,
    embed_bias_ref,
    conv_bias_ref,
    conv_hbm,
    near_ref,
    far_hbm,
    bias_ref,
    edge_ref,
    shift_ref,
    plain_ref,
    left_ref,
    taps_ref,
    made_ref,
    arrived,
    left,
):
    taps = conv_hbm.shape[0]
    near = near_ref.shape[0]
    parts, cells, _ = plain_ref.shape
    depth = cells // PATCH
    rim = left_ref.shape[0] - cells

    def fetch(tap):
        return pltpu.make_async_copy(conv_hbm.at[tap], taps_ref.at[tap], arrived.at[tap])

    def send(tap):
        return pltpu.make_async_copy(made_ref.at[tap], far_hbm.at[tap], left.at[tap])

    for tap in range(taps):
        fetch(tap).start()
    rest = embed_bias_ref[...]
    lines = lax.broadcasted_iota(jnp.int32, (rim, rest.shape[1]), 0)
    below = jnp.zeros(lines.shape, jnp.float32)
    for line in range(3):
        part = rest.astype(left_ref.dtype).astype(jnp.float32)
        below = jnp.where(lines == line, part, below)
        rest = rest - part
    left_ref[cells:] = below.astype(left_ref.dtype)
    for part in range(parts):
        lanes = slice(part * LANES, (part + 1) * LANES)
        plain_ref[part] = embed_ref[..., lanes].astype(jnp.float32).reshape(cells, LANES)
        for step in range(PATCH):
            left_ref[step * depth : (step + 1) * depth, lanes] = plain_ref[
                part, pl.ds(step, depth, stride=PATCH), :
            ].astype(left_ref.dtype)
    shift_ref[...] = jnp.zeros_like(shift_ref)

    def compose(tap, keep):
        fetch(tap).wait()
        both = jnp.dot(left_ref[...], taps_ref[tap], preferred_element_type=jnp.float32)
        shift_ref[tap // 3] += jnp.broadcast_to(
            both[cells:].sum(axis=0, keepdims=True), shift_ref.shape[1:]
        )
        keep(both[:cells].astype(far_hbm.dtype))

    def compose_near(tap, carry):
        def keep(value):
            near_ref[tap] = value

        compose(tap, keep)
        return carry

    def compose_far(tap, carry):
        def keep(value):
            made_ref[tap] = value
            send(tap).start()

        compose(tap + near, keep)
        return carry

    lax.fori_loop(0, near, compose_near, None)
    lax.fori_loop(0, taps - near, compose_far, None)
    lat = lax.axis_index("lat")
    above = jnp.where(lat > 0, 1.0, 0.0).astype(jnp.float32)
    below = jnp.where(lat < lax.axis_size("lat") - 1, 1.0, 0.0).astype(jnp.float32)
    edge_ref[0] = jnp.full(edge_ref.shape[1:], above)
    edge_ref[1] = jnp.full(edge_ref.shape[1:], below)
    middle = conv_bias_ref[...] + shift_ref[1]
    over, under = shift_ref[0], shift_ref[2]
    bias_ref[0] = middle + over * above + under
    bias_ref[1] = middle + over + under
    bias_ref[2] = middle + over + under * below
    for tap in range(taps - near):
        send(tap).wait()


def tokens_kernel(
    tile_ref,
    near_ref,
    far_hbm,
    bias_ref,
    edge_ref,
    out_hbm,
    far_ref,
    turned_ref,
    cells_ref,
    total_ref,
    out_ref,
    arrived,
    left,
    *,
    pitch,
    block,
):
    variables, rows, _, span = tile_ref.shape
    tile_rows, tile_cols, channels = out_ref.shape
    depth = variables * PATCH
    cells = depth * PATCH
    steps = 3 * PATCH
    near = near_ref.shape[0]
    groups = ((near, 3), (3, 4), (4, 6), (6, 9))

    def fetch(group):
        start, stop = groups[group]
        taps = pl.ds(start - near, stop - start)
        return pltpu.make_async_copy(far_hbm.at[taps], far_ref.at[taps], arrived.at[group])

    def send(part):
        lanes = slice(part * block, (part + 1) * block)
        return pltpu.make_async_copy(
            out_ref.at[:, :, lanes], out_hbm.at[:, :, lanes], left.at[part]
        )

    for group in range(len(groups)):
        fetch(group).start()
    for row in range(rows):
        turned = tile_ref[:, row].astype(jnp.float32).reshape(depth, span).T
        if row == 0:
            turned = turned * edge_ref[0, :1]
        if row == rows - 1:
            turned = turned * edge_ref[1, :1]
        turned_ref[row, :span] = turned
        for step in range(steps):
            picked = turned_ref[row, pl.ds(step, pitch, stride=PATCH), :]
            cells_ref[row * pitch : (row + 1) * pitch, step * depth : (step + 1) * depth] = (
                picked.astype(cells_ref.dtype)
            )

    def product(start, weight):
        tap_row, first = divmod(start, 3)
        count = weight.shape[0]
        left = cells_ref[
            tap_row * pitch : (tap_row + tile_rows) * pitch, first * cells : (first + count) * cells
        ]
        right = weight.reshape(count * cells, weight.shape[2])
        return jnp.dot(left, right, preferred_element_type=jnp.float32)

    total_ref[...] = product(0, near_ref[...])
    for group, (start, stop) in enumerate(groups):
        fetch(group).wait()
        if stop < 9:
            total_ref[...] += product(start, far_ref[start - near : stop - near])
    for part in range(channels // block):
        lanes = slice(part * block, (part + 1) * block)
        total = total_ref[:, lanes] + product(start, far_ref[start - near : stop - near, :, lanes])
        for row in range(tile_rows):
            kind = 0 if row == 0 else 2 if row == tile_rows - 1 else 1
            value = total[row * pitch : row * pitch + tile_cols] + bias_ref[kind, :1, lanes]
            value = 0.5 * value * (1.0 + lax.erf(value * (0.5**0.5)))
            out_ref[row, :, lanes] = value.astype(out_ref.dtype)
        send(part).start()
    for part in range(channels // block):
        send(part).wait()


def one_stage(raw_fields, embed_weight, embed_bias, conv_weight, conv_bias):
    lat_count = lax.axis_size("lat")
    lon_count = lax.axis_size("lon")
    devices = lat_count * lon_count
    _, height, breadth = raw_fields.shape
    variables, _, _, channels = embed_weight.shape
    tile_rows = height // lat_count // PATCH
    tile_breadth = breadth // lon_count
    tile_cols = tile_breadth // PATCH
    rows = tile_rows + 2
    span = tile_breadth + 2 * PATCH
    depth = variables * PATCH
    cells = depth * PATCH
    pitch = -(-(tile_cols + 2) // 16) * 16
    lowest = jnp.bfloat16

    pieces = pl.pallas_call(
        functools.partial(
            windows_kernel,
            lat_count=lat_count,
            lon_count=lon_count,
            tile_rows=tile_rows,
            tile_breadth=tile_breadth,
        ),
        out_shape=pltpu.VMEM((devices, rows, PATCH, span), lowest),
        name="windows",
    )(raw_fields)
    tile = lax.all_to_all(pieces, ("lat", "lon"), split_axis=0, concat_axis=0, tiled=True)

    whole = pl.BlockSpec(memory_space=pltpu.VMEM)
    afar = pl.BlockSpec(memory_space=pl.ANY)
    taps, near = 9, 2
    block = channels // 2
    close, far, bias, edge = pl.pallas_call(
        compose_kernel,
        in_specs=[whole, whole, whole, afar],
        out_specs=[whole, afar, whole, whole],
        out_shape=[
            pltpu.VMEM((near, cells, channels), lowest),
            jax.ShapeDtypeStruct((taps - near, cells, channels), lowest),
            pltpu.VMEM((3, 8, channels), jnp.float32),
            pltpu.VMEM((2, 8, depth), jnp.float32),
        ],
        scratch_shapes=[
            pltpu.VMEM((3, 8, channels), jnp.float32),
            pltpu.VMEM((channels // LANES, cells, LANES), jnp.float32),
            pltpu.VMEM((cells + 16, channels), lowest),
            pltpu.VMEM((taps, channels, channels), lowest),
            pltpu.VMEM((taps - near, cells, channels), lowest),
            pltpu.SemaphoreType.DMA((taps,)),
            pltpu.SemaphoreType.DMA((taps - near,)),
        ],
        compiler_params=pltpu.CompilerParams(vmem_limit_bytes=48 << 20),
        name="compose",
    )(
        pltpu.with_memory_space_constraint(embed_weight, pltpu.VMEM),
        embed_bias.reshape(1, channels),
        conv_bias.reshape(1, channels),
        conv_weight.reshape(taps, channels, channels),
    )

    return pl.pallas_call(
        functools.partial(tokens_kernel, pitch=pitch, block=block),
        in_specs=[whole, whole, afar, whole, whole],
        out_specs=afar,
        out_shape=jax.ShapeDtypeStruct((tile_rows, tile_cols, channels), lowest),
        scratch_shapes=[
            pltpu.VMEM((taps - near, cells, channels), lowest),
            pltpu.VMEM((rows, PATCH * pitch + 3 * PATCH, depth), jnp.float32),
            pltpu.VMEM((rows * pitch, 3 * cells), lowest),
            pltpu.VMEM((tile_rows * pitch, channels), jnp.float32),
            pltpu.VMEM((tile_rows, tile_cols, channels), lowest),
            pltpu.SemaphoreType.DMA((4,)),
            pltpu.SemaphoreType.DMA((channels // block,)),
        ],
        compiler_params=pltpu.CompilerParams(vmem_limit_bytes=32 << 20),
        name="tokens",
    )(
        pltpu.with_memory_space_constraint(tile, pltpu.VMEM),
        pltpu.with_memory_space_constraint(close, pltpu.VMEM),
        pltpu.with_memory_space_constraint(far, pltpu.HBM),
        pltpu.with_memory_space_constraint(bias, pltpu.VMEM),
        pltpu.with_memory_space_constraint(edge, pltpu.VMEM),
    )


def per_device(raw_fields, embed_weight, embed_bias, conv_weight, conv_bias):
    variables, _, _, channels = embed_weight.shape
    tile_height = raw_fields.shape[1] // lax.axis_size("lat")
    deep = variables * PATCH * PATCH > channels
    if raw_fields.shape[0] == 1 and tile_height >= 2 * PATCH and not deep:
        return one_stage(raw_fields, embed_weight, embed_bias, conv_weight, conv_bias)
    return two_stages(raw_fields, embed_weight, embed_bias, conv_weight, conv_bias)


def solution(mesh):
    return jax.shard_map(
        per_device,
        mesh=mesh,
        in_specs=(P(("lat", "lon"), None, None), P(), P(), P(), P()),
        out_specs=P("lat", "lon", None),
        check_vma=False,
    )
```

```python
import functools

import jax
import jax.numpy as jnp
from jax import lax
from jax.experimental import pallas as pl
from jax.experimental.pallas import tpu as pltpu
from jax.sharding import PartitionSpec as P

PATCH = 4
LANES = 128


def with_halo(value, sides, width, wrap):
    for axis, dim in sides:
        count, length = (lax.axis_size(axis), value.shape[dim])
        up = [(i, (i + 1) % count) for i in range(count if wrap else count - 1)]
        down = [(j, i) for i, j in up]
        last = lax.slice_in_dim(value, length - width, length, axis=dim)
        leading = lax.slice_in_dim(value, 0, width, axis=dim)
        before = lax.ppermute(last, axis, up)
        after = lax.ppermute(leading, axis, down)
        value = jnp.concatenate([before, value, after], axis=dim)
    return value


def two_stages(raw_fields, embed_weight, embed_bias, conv_weight, conv_bias):
    lat_count = lax.axis_size("lat")
    lon_count = lax.axis_size("lon")
    var_dev, height, breadth = raw_fields.shape
    tile_height = height // lat_count
    tile_breadth = breadth // lon_count
    pieces = raw_fields.reshape(var_dev, lat_count, tile_height, lon_count, tile_breadth)
    pieces = pieces.transpose(1, 3, 0, 2, 4).reshape(
        lat_count * lon_count * var_dev, tile_height, tile_breadth
    )
    tile_block = lax.all_to_all(pieces, ("lat", "lon"), split_axis=0, concat_axis=0, tiled=True)
    patch_rows = tile_height // PATCH
    patch_cols = tile_breadth // PATCH
    grid_blocks = tile_block.reshape(-1, patch_rows, PATCH, patch_cols, PATCH)
    embedded = jnp.einsum(
        "vaibj,vijd->abd", grid_blocks, embed_weight, preferred_element_type=jnp.float32
    )
    embedded = (embedded + embed_bias).astype(jnp.bfloat16)
    channels = embedded.shape[2]
    lon_padded = with_halo(embedded, (("lon", 1),), 1, True)
    padded = with_halo(lon_padded, (("lat", 0),), 1, False)
    summed = jnp.zeros((patch_rows * patch_cols, channels), jnp.float32)
    for step_row in range(3):
        for step_col in range(3):
            window = padded[
                step_row : step_row + patch_rows, step_col : step_col + patch_cols
            ].reshape(-1, channels)
            summed = summed + jnp.dot(
                window, conv_weight[step_row, step_col], preferred_element_type=jnp.float32
            )
    summed = summed + conv_bias
    result = jax.nn.gelu(summed, approximate=False).astype(jnp.bfloat16)
    return result.reshape(patch_rows, patch_cols, channels)


def windows_kernel(raw_ref, out_ref, *, lat_count, lon_count, tile_rows, tile_breadth):
    height, breadth = raw_ref.shape[1:]
    span = tile_breadth + 2 * PATCH
    patches_high = height // PATCH
    rows = tile_rows + 2
    raw = raw_ref[0]
    for lon in range(lon_count):
        first = lon * tile_breadth - PATCH
        last = first + span
        if first < 0:
            window = jnp.concatenate([raw[:, first:], raw[:, :last]], axis=1)
        elif last > breadth:
            window = jnp.concatenate([raw[:, first:], raw[:, : last - breadth]], axis=1)
        else:
            window = raw[:, first:last]
        for patch_row in range(patches_high):
            piece = window[PATCH * patch_row : PATCH * (patch_row + 1)]
            for lat in range(lat_count):
                for step in range(rows):
                    wanted = lat * tile_rows - 1 + step
                    if min(max(wanted, 0), patches_high - 1) == patch_row:
                        out_ref[lat * lon_count + lon, step] = piece


def compose_kernel(
    embed_hbm,
    embed_bias_hbm,
    conv_bias_hbm,
    conv_hbm,
    near_ref,
    far_hbm,
    bias_ref,
    edge_ref,
    embed_ref,
    embed_bias_ref,
    conv_bias_ref,
    shift_ref,
    plain_ref,
    left_ref,
    taps_ref,
    made_ref,
    came,
    arrived,
    left,
):
    taps = conv_hbm.shape[0]
    near = near_ref.shape[0]
    parts, cells, _ = plain_ref.shape
    depth = cells // PATCH
    rim = left_ref.shape[0] - cells

    def fetch(tap):
        return pltpu.make_async_copy(conv_hbm.at[tap], taps_ref.at[tap], arrived.at[tap])

    def send(tap):
        return pltpu.make_async_copy(made_ref.at[tap], far_hbm.at[tap], left.at[tap])

    small = [
        pltpu.make_async_copy(source, target, came.at[place])
        for place, (source, target) in enumerate(
            (
                (embed_bias_hbm, embed_bias_ref),
                (conv_bias_hbm, conv_bias_ref),
                (embed_hbm, embed_ref),
            )
        )
    ]
    for copy in small:
        copy.start()
    for tap in range(taps):
        fetch(tap).start(priority=1)
    for copy in small:
        copy.wait()
    rest = embed_bias_ref[...]
    lines = lax.broadcasted_iota(jnp.int32, (rim, rest.shape[1]), 0)
    below = jnp.zeros(lines.shape, jnp.float32)
    for line in range(3):
        part = rest.astype(left_ref.dtype).astype(jnp.float32)
        below = jnp.where(lines == line, part, below)
        rest = rest - part
    left_ref[cells:] = below.astype(left_ref.dtype)
    for part in range(parts):
        lanes = slice(part * LANES, (part + 1) * LANES)
        plain_ref[part] = embed_ref[..., lanes].astype(jnp.float32).reshape(cells, LANES)
        for step in range(PATCH):
            left_ref[step * depth : (step + 1) * depth, lanes] = plain_ref[
                part, pl.ds(step, depth, stride=PATCH), :
            ].astype(left_ref.dtype)
    shift_ref[...] = jnp.zeros_like(shift_ref)

    def compose(tap, keep):
        fetch(tap).wait()
        both = jnp.dot(left_ref[...], taps_ref[tap], preferred_element_type=jnp.float32)
        shift_ref[tap // 3] += jnp.broadcast_to(
            both[cells:].sum(axis=0, keepdims=True), shift_ref.shape[1:]
        )
        keep(both[:cells].astype(far_hbm.dtype))

    def compose_near(tap, carry):
        def keep(value):
            near_ref[tap] = value

        compose(tap, keep)
        return carry

    def compose_far(tap, carry):
        def keep(value):
            made_ref[tap] = value
            send(tap).start()

        compose(tap + near, keep)
        return carry

    lax.fori_loop(0, near, compose_near, None)
    lax.fori_loop(0, taps - near, compose_far, None)
    lat = lax.axis_index("lat")
    above = jnp.where(lat > 0, 1.0, 0.0).astype(jnp.float32)
    below = jnp.where(lat < lax.axis_size("lat") - 1, 1.0, 0.0).astype(jnp.float32)
    edge_ref[0] = jnp.full(edge_ref.shape[1:], above)
    edge_ref[1] = jnp.full(edge_ref.shape[1:], below)
    middle = conv_bias_ref[...] + shift_ref[1]
    over, under = shift_ref[0], shift_ref[2]
    bias_ref[0] = middle + over * above + under
    bias_ref[1] = middle + over + under
    bias_ref[2] = middle + over + under * below
    for tap in range(taps - near):
        send(tap).wait()


def tokens_kernel(
    tile_ref,
    near_ref,
    far_hbm,
    bias_ref,
    edge_ref,
    out_hbm,
    far_ref,
    turned_ref,
    cells_ref,
    total_ref,
    out_ref,
    arrived,
    left,
    *,
    pitch,
    block,
):
    variables, rows, _, span = tile_ref.shape
    tile_rows, tile_cols, channels = out_ref.shape
    depth = variables * PATCH
    cells = depth * PATCH
    steps = 3 * PATCH
    near = near_ref.shape[0]
    groups = ((near, 3), (3, 4), (4, 6), (6, 9))

    def fetch(group):
        start, stop = groups[group]
        taps = pl.ds(start - near, stop - start)
        return pltpu.make_async_copy(far_hbm.at[taps], far_ref.at[taps], arrived.at[group])

    def send(part):
        lanes = slice(part * block, (part + 1) * block)
        return pltpu.make_async_copy(
            out_ref.at[:, :, lanes], out_hbm.at[:, :, lanes], left.at[part]
        )

    for group in range(len(groups)):
        fetch(group).start()
    for row in range(rows):
        turned = tile_ref[:, row].astype(jnp.float32).reshape(depth, span).T
        if row == 0:
            turned = turned * edge_ref[0, :1]
        if row == rows - 1:
            turned = turned * edge_ref[1, :1]
        turned_ref[row, :span] = turned
        for step in range(steps):
            picked = turned_ref[row, pl.ds(step, pitch, stride=PATCH), :]
            cells_ref[row * pitch : (row + 1) * pitch, step * depth : (step + 1) * depth] = (
                picked.astype(cells_ref.dtype)
            )

    def product(start, weight):
        tap_row, first = divmod(start, 3)
        count = weight.shape[0]
        left = cells_ref[
            tap_row * pitch : (tap_row + tile_rows) * pitch, first * cells : (first + count) * cells
        ]
        right = weight.reshape(count * cells, weight.shape[2])
        return jnp.dot(left, right, preferred_element_type=jnp.float32)

    total_ref[...] = product(0, near_ref[...])
    for group, (start, stop) in enumerate(groups):
        fetch(group).wait()
        if stop < 9:
            total_ref[...] += product(start, far_ref[start - near : stop - near])
    for part in range(channels // block):
        lanes = slice(part * block, (part + 1) * block)
        total = total_ref[:, lanes] + product(start, far_ref[start - near : stop - near, :, lanes])
        for row in range(tile_rows):
            kind = 0 if row == 0 else 2 if row == tile_rows - 1 else 1
            value = total[row * pitch : row * pitch + tile_cols] + bias_ref[kind, :1, lanes]
            value = 0.5 * value * (1.0 + lax.erf(value * (0.5**0.5)))
            out_ref[row, :, lanes] = value.astype(out_ref.dtype)
        send(part).start()
    for part in range(channels // block):
        send(part).wait()


def one_stage(raw_fields, embed_weight, embed_bias, conv_weight, conv_bias):
    lat_count = lax.axis_size("lat")
    lon_count = lax.axis_size("lon")
    devices = lat_count * lon_count
    _, height, breadth = raw_fields.shape
    variables, _, _, channels = embed_weight.shape
    tile_rows = height // lat_count // PATCH
    tile_breadth = breadth // lon_count
    tile_cols = tile_breadth // PATCH
    rows = tile_rows + 2
    span = tile_breadth + 2 * PATCH
    depth = variables * PATCH
    cells = depth * PATCH
    pitch = -(-(tile_cols + 2) // 16) * 16
    lowest = jnp.bfloat16

    pieces = pl.pallas_call(
        functools.partial(
            windows_kernel,
            lat_count=lat_count,
            lon_count=lon_count,
            tile_rows=tile_rows,
            tile_breadth=tile_breadth,
        ),
        out_shape=pltpu.VMEM((devices, rows, PATCH, span), lowest),
        name="windows",
    )(raw_fields)
    tile = lax.all_to_all(pieces, ("lat", "lon"), split_axis=0, concat_axis=0, tiled=True)

    whole = pl.BlockSpec(memory_space=pltpu.VMEM)
    afar = pl.BlockSpec(memory_space=pl.ANY)
    taps, near = 9, 2
    block = channels // 2
    close, far, bias, edge = pl.pallas_call(
        compose_kernel,
        in_specs=[afar] * 4,
        out_specs=[whole, afar, whole, whole],
        out_shape=[
            pltpu.VMEM((near, cells, channels), lowest),
            jax.ShapeDtypeStruct((taps - near, cells, channels), lowest),
            pltpu.VMEM((3, 8, channels), jnp.float32),
            pltpu.VMEM((2, 8, depth), jnp.float32),
        ],
        scratch_shapes=[
            pltpu.VMEM(embed_weight.shape, lowest),
            pltpu.VMEM((1, channels), jnp.float32),
            pltpu.VMEM((1, channels), jnp.float32),
            pltpu.VMEM((3, 8, channels), jnp.float32),
            pltpu.VMEM((channels // LANES, cells, LANES), jnp.float32),
            pltpu.VMEM((cells + 16, channels), lowest),
            pltpu.VMEM((taps, channels, channels), lowest),
            pltpu.VMEM((taps - near, cells, channels), lowest),
            pltpu.SemaphoreType.DMA((3,)),
            pltpu.SemaphoreType.DMA((taps,)),
            pltpu.SemaphoreType.DMA((taps - near,)),
        ],
        compiler_params=pltpu.CompilerParams(vmem_limit_bytes=48 << 20),
        name="compose",
    )(
        *(
            pltpu.with_memory_space_constraint(value, pltpu.HBM)
            for value in (
                embed_weight,
                embed_bias.reshape(1, channels),
                conv_bias.reshape(1, channels),
                conv_weight.reshape(taps, channels, channels),
            )
        )
    )

    return pl.pallas_call(
        functools.partial(tokens_kernel, pitch=pitch, block=block),
        in_specs=[whole, whole, afar, whole, whole],
        out_specs=afar,
        out_shape=jax.ShapeDtypeStruct((tile_rows, tile_cols, channels), lowest),
        scratch_shapes=[
            pltpu.VMEM((taps - near, cells, channels), lowest),
            pltpu.VMEM((rows, PATCH * pitch + 3 * PATCH, depth), jnp.float32),
            pltpu.VMEM((rows * pitch, 3 * cells), lowest),
            pltpu.VMEM((tile_rows * pitch, channels), jnp.float32),
            pltpu.VMEM((tile_rows, tile_cols, channels), lowest),
            pltpu.SemaphoreType.DMA((4,)),
            pltpu.SemaphoreType.DMA((channels // block,)),
        ],
        compiler_params=pltpu.CompilerParams(vmem_limit_bytes=32 << 20),
        name="tokens",
    )(
        pltpu.with_memory_space_constraint(tile, pltpu.VMEM),
        pltpu.with_memory_space_constraint(close, pltpu.VMEM),
        pltpu.with_memory_space_constraint(far, pltpu.HBM),
        pltpu.with_memory_space_constraint(bias, pltpu.VMEM),
        pltpu.with_memory_space_constraint(edge, pltpu.VMEM),
    )


def per_device(raw_fields, embed_weight, embed_bias, conv_weight, conv_bias):
    variables, _, _, channels = embed_weight.shape
    tile_height = raw_fields.shape[1] // lax.axis_size("lat")
    deep = variables * PATCH * PATCH > channels
    if raw_fields.shape[0] == 1 and tile_height >= 2 * PATCH and not deep:
        return one_stage(raw_fields, embed_weight, embed_bias, conv_weight, conv_bias)
    return two_stages(raw_fields, embed_weight, embed_bias, conv_weight, conv_bias)


def solution(mesh):
    return jax.shard_map(
        per_device,
        mesh=mesh,
        in_specs=(P(("lat", "lon"), None, None), P(), P(), P(), P()),
        out_specs=P("lat", "lon", None),
        check_vma=False,
    )
```

```python
import functools

import jax
import jax.numpy as jnp
from jax import lax
from jax.experimental import pallas as pl
from jax.experimental.pallas import tpu as pltpu
from jax.sharding import PartitionSpec as P

PATCH = 4
LANES = 128


def with_halo(value, sides, width, wrap):
    for axis, dim in sides:
        count, length = (lax.axis_size(axis), value.shape[dim])
        up = [(i, (i + 1) % count) for i in range(count if wrap else count - 1)]
        down = [(j, i) for i, j in up]
        last = lax.slice_in_dim(value, length - width, length, axis=dim)
        leading = lax.slice_in_dim(value, 0, width, axis=dim)
        before = lax.ppermute(last, axis, up)
        after = lax.ppermute(leading, axis, down)
        value = jnp.concatenate([before, value, after], axis=dim)
    return value


def two_stages(raw_fields, embed_weight, embed_bias, conv_weight, conv_bias):
    lat_count = lax.axis_size("lat")
    lon_count = lax.axis_size("lon")
    var_dev, height, breadth = raw_fields.shape
    tile_height = height // lat_count
    tile_breadth = breadth // lon_count
    pieces = raw_fields.reshape(var_dev, lat_count, tile_height, lon_count, tile_breadth)
    pieces = pieces.transpose(1, 3, 0, 2, 4).reshape(
        lat_count * lon_count * var_dev, tile_height, tile_breadth
    )
    tile_block = lax.all_to_all(pieces, ("lat", "lon"), split_axis=0, concat_axis=0, tiled=True)
    patch_rows = tile_height // PATCH
    patch_cols = tile_breadth // PATCH
    grid_blocks = tile_block.reshape(-1, patch_rows, PATCH, patch_cols, PATCH)
    embedded = jnp.einsum(
        "vaibj,vijd->abd", grid_blocks, embed_weight, preferred_element_type=jnp.float32
    )
    embedded = (embedded + embed_bias).astype(jnp.bfloat16)
    channels = embedded.shape[2]
    lon_padded = with_halo(embedded, (("lon", 1),), 1, True)
    padded = with_halo(lon_padded, (("lat", 0),), 1, False)
    summed = jnp.zeros((patch_rows * patch_cols, channels), jnp.float32)
    for step_row in range(3):
        for step_col in range(3):
            window = padded[
                step_row : step_row + patch_rows, step_col : step_col + patch_cols
            ].reshape(-1, channels)
            summed = summed + jnp.dot(
                window, conv_weight[step_row, step_col], preferred_element_type=jnp.float32
            )
    summed = summed + conv_bias
    result = jax.nn.gelu(summed, approximate=False).astype(jnp.bfloat16)
    return result.reshape(patch_rows, patch_cols, channels)


def windows_kernel(
    raw_hbm, out_hbm, raw_ref, out_ref, arrived, left, *, lat_count, lon_count, tile_rows
):
    height, breadth = raw_ref.shape
    _, rows, _, span = out_ref.shape
    tile_breadth = breadth // lon_count
    patches_high = height // PATCH
    pieces = arrived.shape[0]
    share = height // pieces

    def fetch(piece):
        lines = pl.ds(piece * share, share)
        return pltpu.make_async_copy(raw_hbm.at[0, lines], raw_ref.at[lines], arrived.at[piece])

    def send(lat):
        tiles = pl.ds(lat * lon_count, lon_count)
        return pltpu.make_async_copy(out_ref.at[tiles], out_hbm.at[tiles], left.at[lat])

    def wanted(lat, step):
        return min(max(lat * tile_rows - 1 + step, 0), patches_high - 1)

    for piece in range(pieces):
        fetch(piece).start()
    for piece in range(pieces):
        fetch(piece).wait()
        raw = raw_ref[piece * share : (piece + 1) * share]
        low, high = piece * share // PATCH, (piece + 1) * share // PATCH
        for lon in range(lon_count):
            first = lon * tile_breadth - PATCH
            last = first + span
            if first < 0:
                window = jnp.concatenate([raw[:, first:], raw[:, :last]], axis=1)
            elif last > breadth:
                window = jnp.concatenate([raw[:, first:], raw[:, : last - breadth]], axis=1)
            else:
                window = raw[:, first:last]
            for lat in range(lat_count):
                for step in range(rows):
                    row = wanted(lat, step)
                    if low <= row < high:
                        start = PATCH * (row - low)
                        out_ref[lat * lon_count + lon, step] = window[start : start + PATCH]
        for lat in range(lat_count):
            if low <= wanted(lat, rows - 1) < high:
                send(lat).start()
    for lat in range(lat_count):
        send(lat).wait()


def compose_kernel(
    embed_hbm,
    embed_bias_hbm,
    conv_bias_hbm,
    conv_hbm,
    near_ref,
    far_hbm,
    bias_ref,
    edge_ref,
    embed_ref,
    embed_bias_ref,
    conv_bias_ref,
    shift_ref,
    plain_ref,
    left_ref,
    taps_ref,
    made_ref,
    came,
    arrived,
    left,
):
    taps = conv_hbm.shape[0]
    near = near_ref.shape[0]
    parts, cells, _ = plain_ref.shape
    depth = cells // PATCH
    rim = left_ref.shape[0] - cells

    def fetch(tap):
        return pltpu.make_async_copy(conv_hbm.at[tap], taps_ref.at[tap], arrived.at[tap])

    def send(tap):
        return pltpu.make_async_copy(made_ref.at[tap], far_hbm.at[tap], left.at[tap])

    small = [
        pltpu.make_async_copy(source, target, came.at[place])
        for place, (source, target) in enumerate(
            (
                (embed_bias_hbm, embed_bias_ref),
                (conv_bias_hbm, conv_bias_ref),
                (embed_hbm, embed_ref),
            )
        )
    ]
    for copy in small:
        copy.start()
    for tap in range(taps):
        fetch(tap).start(priority=1)
    for copy in small:
        copy.wait()
    rest = embed_bias_ref[...]
    lines = lax.broadcasted_iota(jnp.int32, (rim, rest.shape[1]), 0)
    below = jnp.zeros(lines.shape, jnp.float32)
    for line in range(3):
        part = rest.astype(left_ref.dtype).astype(jnp.float32)
        below = jnp.where(lines == line, part, below)
        rest = rest - part
    left_ref[cells:] = below.astype(left_ref.dtype)
    for part in range(parts):
        lanes = slice(part * LANES, (part + 1) * LANES)
        plain_ref[part] = embed_ref[..., lanes].astype(jnp.float32).reshape(cells, LANES)
        for step in range(PATCH):
            left_ref[step * depth : (step + 1) * depth, lanes] = plain_ref[
                part, pl.ds(step, depth, stride=PATCH), :
            ].astype(left_ref.dtype)
    shift_ref[...] = jnp.zeros_like(shift_ref)

    def compose(tap, keep):
        fetch(tap).wait()
        both = jnp.dot(left_ref[...], taps_ref[tap], preferred_element_type=jnp.float32)
        shift_ref[tap // 3] += jnp.broadcast_to(
            both[cells:].sum(axis=0, keepdims=True), shift_ref.shape[1:]
        )
        keep(both[:cells].astype(far_hbm.dtype))

    def compose_near(tap, carry):
        def keep(value):
            near_ref[tap] = value

        compose(tap, keep)
        return carry

    def compose_far(tap, carry):
        def keep(value):
            made_ref[tap] = value
            send(tap).start()

        compose(tap + near, keep)
        return carry

    lax.fori_loop(0, near, compose_near, None)
    lax.fori_loop(0, taps - near, compose_far, None)
    lat = lax.axis_index("lat")
    above = jnp.where(lat > 0, 1.0, 0.0).astype(jnp.float32)
    below = jnp.where(lat < lax.axis_size("lat") - 1, 1.0, 0.0).astype(jnp.float32)
    edge_ref[0] = jnp.full(edge_ref.shape[1:], above)
    edge_ref[1] = jnp.full(edge_ref.shape[1:], below)
    middle = conv_bias_ref[...] + shift_ref[1]
    over, under = shift_ref[0], shift_ref[2]
    bias_ref[0] = middle + over * above + under
    bias_ref[1] = middle + over + under
    bias_ref[2] = middle + over + under * below
    for tap in range(taps - near):
        send(tap).wait()


def tokens_kernel(
    tile_ref,
    near_ref,
    far_hbm,
    bias_ref,
    edge_ref,
    out_hbm,
    far_ref,
    turned_ref,
    cells_ref,
    total_ref,
    out_ref,
    arrived,
    left,
    *,
    pitch,
    block,
):
    variables, rows, _, span = tile_ref.shape
    tile_rows, tile_cols, channels = out_ref.shape
    depth = variables * PATCH
    cells = depth * PATCH
    steps = 3 * PATCH
    near = near_ref.shape[0]
    groups = ((near, 3), (3, 4), (4, 6), (6, 9))

    def fetch(group):
        start, stop = groups[group]
        taps = pl.ds(start - near, stop - start)
        return pltpu.make_async_copy(far_hbm.at[taps], far_ref.at[taps], arrived.at[group])

    def send(part):
        lanes = slice(part * block, (part + 1) * block)
        return pltpu.make_async_copy(
            out_ref.at[:, :, lanes], out_hbm.at[:, :, lanes], left.at[part]
        )

    for group in range(len(groups)):
        fetch(group).start()
    for row in range(rows):
        turned = tile_ref[:, row].astype(jnp.float32).reshape(depth, span).T
        if row == 0:
            turned = turned * edge_ref[0, :1]
        if row == rows - 1:
            turned = turned * edge_ref[1, :1]
        turned_ref[row, :span] = turned
        for step in range(steps):
            picked = turned_ref[row, pl.ds(step, pitch, stride=PATCH), :]
            cells_ref[row * pitch : (row + 1) * pitch, step * depth : (step + 1) * depth] = (
                picked.astype(cells_ref.dtype)
            )

    def product(start, weight):
        tap_row, first = divmod(start, 3)
        count = weight.shape[0]
        left = cells_ref[
            tap_row * pitch : (tap_row + tile_rows) * pitch, first * cells : (first + count) * cells
        ]
        right = weight.reshape(count * cells, weight.shape[2])
        return jnp.dot(left, right, preferred_element_type=jnp.float32)

    total_ref[...] = product(0, near_ref[...])
    for group, (start, stop) in enumerate(groups):
        fetch(group).wait()
        if stop < 9:
            total_ref[...] += product(start, far_ref[start - near : stop - near])
    for part in range(channels // block):
        lanes = slice(part * block, (part + 1) * block)
        total = total_ref[:, lanes] + product(start, far_ref[start - near : stop - near, :, lanes])
        for row in range(tile_rows):
            kind = 0 if row == 0 else 2 if row == tile_rows - 1 else 1
            value = total[row * pitch : row * pitch + tile_cols] + bias_ref[kind, :1, lanes]
            value = 0.5 * value * (1.0 + lax.erf(value * (0.5**0.5)))
            out_ref[row, :, lanes] = value.astype(out_ref.dtype)
        send(part).start()
    for part in range(channels // block):
        send(part).wait()


def one_stage(raw_fields, embed_weight, embed_bias, conv_weight, conv_bias):
    lat_count = lax.axis_size("lat")
    lon_count = lax.axis_size("lon")
    devices = lat_count * lon_count
    _, height, breadth = raw_fields.shape
    variables, _, _, channels = embed_weight.shape
    tile_rows = height // lat_count // PATCH
    tile_breadth = breadth // lon_count
    tile_cols = tile_breadth // PATCH
    rows = tile_rows + 2
    span = tile_breadth + 2 * PATCH
    depth = variables * PATCH
    cells = depth * PATCH
    pitch = -(-(tile_cols + 2) // 16) * 16
    lowest = jnp.bfloat16

    halves = 2 if height % (4 * PATCH) == 0 else 1
    pieces = pl.pallas_call(
        functools.partial(
            windows_kernel, lat_count=lat_count, lon_count=lon_count, tile_rows=tile_rows
        ),
        in_specs=[pl.BlockSpec(memory_space=pl.ANY)],
        out_specs=pl.BlockSpec(memory_space=pl.ANY),
        out_shape=jax.ShapeDtypeStruct((devices, rows, PATCH, span), lowest),
        scratch_shapes=[
            pltpu.VMEM((height, breadth), lowest),
            pltpu.VMEM((devices, rows, PATCH, span), lowest),
            pltpu.SemaphoreType.DMA((halves,)),
            pltpu.SemaphoreType.DMA((lat_count,)),
        ],
        name="windows",
    )(pltpu.with_memory_space_constraint(raw_fields, pltpu.HBM))
    tile = lax.all_to_all(pieces, ("lat", "lon"), split_axis=0, concat_axis=0, tiled=True)

    whole = pl.BlockSpec(memory_space=pltpu.VMEM)
    afar = pl.BlockSpec(memory_space=pl.ANY)
    taps, near = 9, 2
    block = channels // 2
    close, far, bias, edge = pl.pallas_call(
        compose_kernel,
        in_specs=[afar] * 4,
        out_specs=[whole, afar, whole, whole],
        out_shape=[
            pltpu.VMEM((near, cells, channels), lowest),
            jax.ShapeDtypeStruct((taps - near, cells, channels), lowest),
            pltpu.VMEM((3, 8, channels), jnp.float32),
            pltpu.VMEM((2, 8, depth), jnp.float32),
        ],
        scratch_shapes=[
            pltpu.VMEM(embed_weight.shape, lowest),
            pltpu.VMEM((1, channels), jnp.float32),
            pltpu.VMEM((1, channels), jnp.float32),
            pltpu.VMEM((3, 8, channels), jnp.float32),
            pltpu.VMEM((channels // LANES, cells, LANES), jnp.float32),
            pltpu.VMEM((cells + 16, channels), lowest),
            pltpu.VMEM((taps, channels, channels), lowest),
            pltpu.VMEM((taps - near, cells, channels), lowest),
            pltpu.SemaphoreType.DMA((3,)),
            pltpu.SemaphoreType.DMA((taps,)),
            pltpu.SemaphoreType.DMA((taps - near,)),
        ],
        compiler_params=pltpu.CompilerParams(vmem_limit_bytes=48 << 20),
        name="compose",
    )(
        *(
            pltpu.with_memory_space_constraint(value, pltpu.HBM)
            for value in (
                embed_weight,
                embed_bias.reshape(1, channels),
                conv_bias.reshape(1, channels),
                conv_weight.reshape(taps, channels, channels),
            )
        )
    )

    return pl.pallas_call(
        functools.partial(tokens_kernel, pitch=pitch, block=block),
        in_specs=[whole, whole, afar, whole, whole],
        out_specs=afar,
        out_shape=jax.ShapeDtypeStruct((tile_rows, tile_cols, channels), lowest),
        scratch_shapes=[
            pltpu.VMEM((taps - near, cells, channels), lowest),
            pltpu.VMEM((rows, PATCH * pitch + 3 * PATCH, depth), jnp.float32),
            pltpu.VMEM((rows * pitch, 3 * cells), lowest),
            pltpu.VMEM((tile_rows * pitch, channels), jnp.float32),
            pltpu.VMEM((tile_rows, tile_cols, channels), lowest),
            pltpu.SemaphoreType.DMA((4,)),
            pltpu.SemaphoreType.DMA((channels // block,)),
        ],
        compiler_params=pltpu.CompilerParams(vmem_limit_bytes=32 << 20),
        name="tokens",
    )(
        pltpu.with_memory_space_constraint(tile, pltpu.VMEM),
        pltpu.with_memory_space_constraint(close, pltpu.VMEM),
        pltpu.with_memory_space_constraint(far, pltpu.HBM),
        pltpu.with_memory_space_constraint(bias, pltpu.VMEM),
        pltpu.with_memory_space_constraint(edge, pltpu.VMEM),
    )


def per_device(raw_fields, embed_weight, embed_bias, conv_weight, conv_bias):
    variables, _, _, channels = embed_weight.shape
    tile_height = raw_fields.shape[1] // lax.axis_size("lat")
    deep = variables * PATCH * PATCH > channels
    if raw_fields.shape[0] == 1 and tile_height >= 2 * PATCH and not deep:
        return one_stage(raw_fields, embed_weight, embed_bias, conv_weight, conv_bias)
    return two_stages(raw_fields, embed_weight, embed_bias, conv_weight, conv_bias)


def solution(mesh):
    return jax.shard_map(
        per_device,
        mesh=mesh,
        in_specs=(P(("lat", "lon"), None, None), P(), P(), P(), P()),
        out_specs=P("lat", "lon", None),
        check_vma=False,
    )
```
